32 devices in a mesh: dp: 4 (over y, x), ep: 8 (over z, core).
Axes of the slice: x: 2, y: 2, z: 4, core: 2. Of those that a mesh axis runs over, the one named last changes fastest.
Arguments:
- tokens: bfloat16 [4096, 7168], P(('dp', 'ep')), may hold values from -6 to 6
- out_grad: bfloat16 [4096, 7168], P(('dp', 'ep')), may hold values from -3 to 3
- route_weight: float32 [4096, 1], P(('dp', 'ep')), may hold values from 0.2 to 1
- expert_ids: int32 [4096, 1], P(('dp', 'ep')), may hold values from 0 to 1
- w_gate: bfloat16 [1024, 14336], P('dp', 'ep'), may hold values from -0.0625 to 0.0625
- w_up: bfloat16 [1024, 14336], P('dp', 'ep'), may hold values from -0.0625 to 0.0625
- w_down: bfloat16 [1024, 14336], P('dp', 'ep'), may hold values from -0.1875 to 0.1875
Outputs:
- in_grad: bfloat16 [4096, 7168], P(('dp', 'ep'))
- grad_gate: bfloat16 [1024, 14336], P('dp', 'ep')
- grad_up: bfloat16 [1024, 14336], P('dp', 'ep')
- grad_down: bfloat16 [1024, 14336], P('dp', 'ep')
The draws below stay inside these ranges and needn't reach their ends.
All inputs are finite; a program needn't handle non-finite values.
Results may differ from the reference program's by a relative error of at most 0.012.
Values may be sent and summed in bfloat16 or wider, within the bound.
A program may use at most 128 MiB of HBM per device.

```python
import jax
import jax.numpy as jnp
from jax import lax

D = 7168
FF = 1024
GROUP = 4
TOP = 1
TOK_DEV = 128
EXPERTS = 2
CAP = 48
TOKENS = 4096
N_DP = 4
N_EP = 8


def shard_levels(key, dims, pieces, low, top_value):
    factor_of, own = 1.0, jax.random.fold_in(key, 6)
    for dim, parts in pieces:
        heights = jnp.exp(jax.random.uniform(jax.random.fold_in(own, dim), (parts,), jnp.float32, low / len(pieces), top_value / len(pieces)))
        factor_of = factor_of * jnp.repeat(heights, dims[dim] // parts).reshape([-1 if axis == dim else 1 for axis in range(len(dims))])
    return factor_of


def picks_of(own_key, rows, count, top, lift):
    sequence = jax.random.permutation(jax.random.fold_in(own_key, 1), count)
    pull = sequence
    for power in range(3):
        pull = pull * pull // count
    pull = pull * lift // count
    chance = jax.random.randint(jax.random.fold_in(own_key, 2), (rows, count), 0, 4096) + pull
    fixed_rows = jax.random.permutation(jax.random.fold_in(own_key, 3), rows)[jnp.arange(count) % rows]
    chance = jnp.where(jnp.arange(rows)[:, None] == fixed_rows[None, :], 1 << 14, chance)
    score = chance * count + jnp.arange(count)
    return lax.top_k(score.astype(jnp.int32), top)[1].astype(jnp.int32)


def centred(rng, dims, width, most, cuts=(), held_as=jnp.bfloat16):
    drawn = width * jax.random.normal(rng, dims, jnp.float32)
    if cuts:
        drawn = drawn * shard_levels(rng, dims, cuts, -0.22, 0.18)
    return jnp.clip(drawn, -most, most).astype(held_as)


def setup_inputs(seed: int = 0) -> dict:
    splits = jax.random.split(jax.random.key(seed), 8)
    tokens = centred(splits[0], (TOKENS, D), 1.0, 6.0, ((0, 32),))
    out_grad = centred(splits[1], (TOKENS, D), 0.5, 3.0, ((0, 32),))
    route_weight = jnp.clip(0.2 + 0.8 * jax.random.uniform(splits[2], (TOKENS, TOP), jnp.float32) ** shard_levels(splits[2], (TOKENS, TOP), ((0, 32),), -0.2, 0.2), 0.2, 1.0)
    expert_ids = picks_of(splits[3], TOKENS, EXPERTS, TOP, 8192)
    w_gate = centred(splits[4], (FF, EXPERTS * D), D ** -0.5, 0.0625, ((0, 4), (1, 8)))
    w_up = centred(splits[5], (FF, EXPERTS * D), D ** -0.5, 0.0625, ((0, 4), (1, 8)))
    w_down = centred(splits[6], (FF, EXPERTS * D), FF ** -0.5, 0.1875, ((0, 4), (1, 8)))
    return {"tokens": tokens, "out_grad": out_grad, "route_weight": route_weight, "expert_ids": expert_ids, "w_gate": w_gate, "w_up": w_up, "w_down": w_down}


CONTRACT_LAST = (((1,), (1,)), ((), ()))
CONTRACT_FIRST = (((0,), (0,)), ((), ()))


def slot_tables(expert_ids, route_weight, experts, capacity):
    token_count, top_count = expert_ids.shape
    pair_count = token_count * top_count
    flat_ids = expert_ids.reshape(pair_count)
    onehot = (flat_ids[:, None] == jnp.arange(experts, dtype=jnp.int32)[None, :]).astype(jnp.int32)
    before = jnp.cumsum(onehot, axis=0) - onehot
    ranks = jnp.sum(before * onehot, axis=1)
    kept = ranks < capacity
    slots = jnp.where(kept, flat_ids * capacity + ranks, 0).astype(jnp.int32)
    slot_ids = jnp.arange(experts * capacity, dtype=jnp.int32)
    match = (slots[None, :] == slot_ids[:, None]) & kept[None, :]
    pair_ids = jnp.arange(pair_count, dtype=jnp.int32)
    pair_of_slot = jnp.sum(jnp.where(match, pair_ids[None, :], 0), axis=1).astype(jnp.int32)
    filled = jnp.any(match, axis=1)
    flat_weight = route_weight.reshape(pair_count)
    weight_of_slot = jnp.sum(jnp.where(match, flat_weight[None, :], jnp.float32(0.0)), axis=1)
    return kept, slots, pair_of_slot // top_count, filled, weight_of_slot


def source_slots(tokens, out_grad, route_weight, expert_ids):
    kept, slots, token_of_slot, filled, weight_of_slot = slot_tables(expert_ids, route_weight, EXPERTS, CAP)
    x_slots = jnp.take(tokens, token_of_slot, axis=0) * filled[:, None].astype(jnp.bfloat16)
    d_slots = (jnp.take(out_grad, token_of_slot, axis=0).astype(jnp.float32) * weight_of_slot[:, None]).astype(jnp.bfloat16)
    return x_slots, d_slots, kept, slots


def quarter_sum(left, weight):
    quarter = D // GROUP
    total = jnp.zeros((left.shape[0], weight.shape[0]), jnp.float32)
    for piece in range(GROUP):
        part = lax.dot_general(left[:, piece * quarter:(piece + 1) * quarter], weight[:, piece * quarter:(piece + 1) * quarter], CONTRACT_LAST, preferred_element_type=jnp.float32)
        total = total + lax.optimization_barrier(part.astype(jnp.bfloat16)).astype(jnp.float32)
    return total


def activations(gate, up, back):
    logistic = jax.nn.sigmoid(gate)
    silu = gate * logistic
    hidden = (silu * up).astype(jnp.bfloat16)
    d_gate = (back * up * logistic * (1.0 + gate * (1.0 - logistic))).astype(jnp.bfloat16)
    d_up = (back * silu).astype(jnp.bfloat16)
    return hidden, d_gate, d_up


def expert_work(operands):
    x_rows, d_rows, gate_w, up_w, down_w = operands
    gate = quarter_sum(x_rows, gate_w)
    up = quarter_sum(x_rows, up_w)
    back = quarter_sum(d_rows, down_w)
    hidden, d_gate, d_up = activations(gate, up, back)
    expert_dx = (jnp.dot(d_gate, gate_w, preferred_element_type=jnp.float32) + jnp.dot(d_up, up_w, preferred_element_type=jnp.float32)).astype(jnp.bfloat16)
    gate_term = lax.dot_general(d_gate, x_rows, CONTRACT_FIRST, preferred_element_type=jnp.float32).astype(jnp.bfloat16)
    up_term = lax.dot_general(d_up, x_rows, CONTRACT_FIRST, preferred_element_type=jnp.float32).astype(jnp.bfloat16)
    down_term = lax.dot_general(hidden, d_rows, CONTRACT_FIRST, preferred_element_type=jnp.float32).astype(jnp.bfloat16)
    return expert_dx, gate_term, up_term, down_term


def reference(tokens, out_grad, route_weight, expert_ids, w_gate, w_up, w_down):
    sources = N_DP * N_EP
    x_src = tokens.reshape(sources, TOK_DEV, D)
    d_src = out_grad.reshape(sources, TOK_DEV, D)
    w_src = route_weight.reshape(sources, TOK_DEV, TOP)
    i_src = expert_ids.reshape(sources, TOK_DEV, TOP)
    x_slots, d_slots, kept, slots = jax.vmap(source_slots)(x_src, d_src, w_src, i_src)
    x_slots = x_slots.reshape(N_DP, N_EP, EXPERTS, CAP, D)
    d_slots = d_slots.reshape(N_DP, N_EP, EXPERTS, CAP, D)
    gate_e = w_gate.reshape(FF, EXPERTS, D).transpose(1, 0, 2)
    up_e = w_up.reshape(FF, EXPERTS, D).transpose(1, 0, 2)
    down_e = w_down.reshape(FF, EXPERTS, D).transpose(1, 0, 2)
    grad_sums = [jnp.zeros((EXPERTS, FF, D), jnp.float32) for which in range(3)]
    returned = []
    for row in range(N_DP):
        x_rows = x_slots[row].transpose(1, 0, 2, 3).reshape(EXPERTS, N_EP * CAP, D)
        d_rows = d_slots[row].transpose(1, 0, 2, 3).reshape(EXPERTS, N_EP * CAP, D)
        expert_dx, gate_term, up_term, down_term = lax.map(expert_work, (x_rows, d_rows, gate_e, up_e, down_e))
        grad_sums = [grad_sums[0] + gate_term.astype(jnp.float32), grad_sums[1] + up_term.astype(jnp.float32), grad_sums[2] + down_term.astype(jnp.float32)]
        returned.append(expert_dx.reshape(EXPERTS, N_EP, CAP, D).transpose(1, 0, 2, 3).reshape(N_EP, EXPERTS * CAP, D))
    slot_rows = jnp.stack(returned, axis=0).reshape(sources, EXPERTS * CAP, D)

    def gather_back(rows, kept_one, slots_one):
        pair_rows = jnp.take(rows, slots_one, axis=0) * kept_one[:, None].astype(jnp.bfloat16)
        return jnp.sum(pair_rows.reshape(TOK_DEV, TOP, D).astype(jnp.float32), axis=1).astype(jnp.bfloat16)

    in_grad = jax.vmap(gather_back)(slot_rows, kept, slots).reshape(TOK_DEV * sources, D)
    outs = [total.astype(jnp.bfloat16).transpose(1, 0, 2).reshape(FF, EXPERTS * D) for total in grad_sums]
    return in_grad, outs[0], outs[1], outs[2]
```

```python
import jax
import jax.numpy as jnp
from jax import lax
from jax.sharding import PartitionSpec as P

D = 7168
GROUP = 4
TOP = 1


CONTRACT_LAST = (((1,), (1,)), ((), ()))
CONTRACT_FIRST = (((0,), (0,)), ((), ()))


def as_sent(value):

    def short(part):
        return part.astype(jnp.bfloat16) if part.dtype == jnp.float32 else part

    return jax.tree.map(short, value)


def from_partner(value, axis, distance):
    mask = 2**distance
    pairs = [(source, source ^ mask) for source in range(lax.axis_size(axis))]
    return lax.ppermute(value, axis, pairs)


def slot_tables(expert_ids, route_weight, experts, capacity):
    token_count, top_count = expert_ids.shape
    pair_count = token_count * top_count
    flat_ids = expert_ids.reshape(pair_count)
    onehot = (flat_ids[:, None] == jnp.arange(experts, dtype=jnp.int32)[None, :]).astype(jnp.int32)
    before = jnp.cumsum(onehot, axis=0) - onehot
    ranks = jnp.sum(before * onehot, axis=1)
    kept = ranks < capacity
    slots = jnp.where(kept, flat_ids * capacity + ranks, 0)
    slot_ids = jnp.arange(experts * capacity, dtype=jnp.int32)
    match = (slots[None, :] == slot_ids[:, None]) & kept[None, :]
    pair_ids = jnp.arange(pair_count, dtype=jnp.int32)
    pair_of_slot = jnp.sum(jnp.where(match, pair_ids[None, :], 0), axis=1)
    filled = jnp.any(match, axis=1)
    flat_weight = route_weight.reshape(pair_count)
    weight_of_slot = jnp.sum(jnp.where(match, flat_weight[None, :], jnp.float32(0.0)), axis=1)
    return (kept, slots, pair_of_slot // top_count, filled, weight_of_slot)


def activations(gate, up, back):
    logistic = jax.nn.sigmoid(gate)
    silu = gate * logistic
    hidden = (silu * up).astype(jnp.bfloat16)
    d_gate = (back * up * logistic * (1.0 + gate * (1.0 - logistic))).astype(jnp.bfloat16)
    d_up = (back * silu).astype(jnp.bfloat16)
    return (hidden, d_gate, d_up)


def swap(value, axis, distance):
    return from_partner(value, axis, distance)


def wide(value):
    return value.astype(jnp.float32)


def dot_last(left, right):
    return lax.dot_general(left, right, CONTRACT_LAST, preferred_element_type=jnp.float32)


def dot_first(left, right):
    return lax.dot_general(left, right, CONTRACT_FIRST, preferred_element_type=jnp.float32)


def body(tokens, out_grad, route_weight, expert_ids, w_gate, w_up, w_down):
    devices_ep = lax.axis_size("ep")
    experts = devices_ep // GROUP
    token_count = tokens.shape[0]
    capacity = 6 * GROUP * token_count * TOP // (8 * devices_ep)
    quarter = D // GROUP
    short = jnp.bfloat16
    kept, slots, token_of_slot, filled, weight_of_slot = slot_tables(
        expert_ids, route_weight, experts, capacity
    )
    other_w = tuple(swap(w, "dp", 1) for w in (w_gate, w_up, w_down))
    token_ids = jnp.arange(token_count, dtype=jnp.int32)
    pick = ((token_of_slot[:, None] == token_ids[None, :]) & filled[:, None]).astype(short)
    x_slots = jnp.dot(pick, tokens, preferred_element_type=jnp.float32).astype(short)
    d_slots = (
        jnp.dot(pick, out_grad, preferred_element_type=jnp.float32) * weight_of_slot[:, None]
    ).astype(short)

    def to_owners(rows):
        shaped = rows.reshape(experts, capacity, GROUP, quarter).transpose(0, 2, 1, 3)
        return shaped.reshape(devices_ep, capacity, quarter)

    def sent(rows):
        return lax.all_to_all(to_owners(rows), "ep", split_axis=0, concat_axis=0, tiled=True)

    row_count = devices_ep * capacity
    x_own = sent(x_slots).reshape(row_count, quarter)
    d_own = sent(d_slots).reshape(row_count, quarter)
    x_other, d_other = swap(x_own, "dp", 0), swap(d_own, "dp", 0)
    core = lax.axis_index("ep") % 2
    weights = ((w_gate, w_up, w_down), other_w)
    acts = []
    for x_rows, d_rows in ((x_own, d_own), (x_other, d_other)):
        terms = [
            jnp.concatenate(
                [dot_last(x_rows, wg), dot_last(x_rows, wu), dot_last(d_rows, wd)], axis=1
            ).astype(short)
            for wg, wu, wd in weights
        ]
        give = jnp.where(core == 0, terms[1], terms[0])
        keep = jnp.where(core == 0, terms[0], terms[1])
        pair = (wide(keep) + wide(swap(give, "ep", 0))).astype(short)
        total = wide(pair) + wide(swap(pair, "ep", 1))
        width = total.shape[1] // 3
        mine = jnp.concatenate(
            activations(total[:, :width], total[:, width : 2 * width], total[:, 2 * width :]), axis=1
        )
        theirs = swap(mine, "ep", 0)
        first = jnp.where(core == 0, mine, theirs)
        second = jnp.where(core == 0, theirs, mine)
        acts.append(
            tuple(
                tuple(half[:, piece * width : (piece + 1) * width] for piece in range(3))
                for half in (first, second)
            )
        )

    def grads(half):
        (h0, g0, u0), (h1, g1, u1) = acts[0][half], acts[1][half]
        return (
            dot_first(g0, x_own) + dot_first(g1, x_other),
            dot_first(u0, x_own) + dot_first(u1, x_other),
            dot_first(h0, d_own) + dot_first(h1, d_other),
        )

    def dx(rows):
        return sum(
            jnp.dot(acts[rows][half][1], weights[half][0], preferred_element_type=jnp.float32)
            + jnp.dot(acts[rows][half][2], weights[half][1], preferred_element_type=jnp.float32)
            for half in range(2)
        )

    dx_in = swap(dx(1).astype(short), "dp", 0)
    away = tuple(swap(term.astype(short), "dp", 1) for term in grads(1))
    expert_dx = (dx(0) + wide(dx_in)).astype(short)
    grad_gate, grad_up, grad_down = (
        (own + wide(term)).astype(short) for own, term in zip(grads(0), away)
    )
    returned = lax.all_to_all(
        expert_dx.reshape(devices_ep, capacity, quarter),
        "ep",
        split_axis=0,
        concat_axis=0,
        tiled=True,
    )
    slot_rows = (
        returned.reshape(experts, GROUP, capacity, quarter)
        .transpose(0, 2, 1, 3)
        .reshape(experts * capacity, D)
    )
    in_grad = dot_first(pick, slot_rows).astype(short)
    return (in_grad, grad_gate, grad_up, grad_down)


def solution(mesh):
    placed = (
        P(("dp", "ep"), None),
        P(("dp", "ep"), None),
        P(("dp", "ep"), None),
        P(("dp", "ep"), None),
        P("dp", "ep"),
        P("dp", "ep"),
        P("dp", "ep"),
    )
    return jax.shard_map(
        body,
        mesh=mesh,
        in_specs=placed,
        out_specs=(P(("dp", "ep"), None), P("dp", "ep"), P("dp", "ep"), P("dp", "ep")),
        check_vma=False,
    )
```

```python
import jax
import jax.numpy as jnp
from jax import lax
from jax.experimental import pallas as pl
from jax.experimental.pallas import tpu as pltpu
from jax.sharding import PartitionSpec as P

D = 7168
GROUP = 4
TOP = 1


CONTRACT_LAST = (((1,), (1,)), ((), ()))
CONTRACT_FIRST = (((0,), (0,)), ((), ()))


def as_sent(value):

    def short(part):
        return part.astype(jnp.bfloat16) if part.dtype == jnp.float32 else part

    return jax.tree.map(short, value)


def from_partner(value, axis, distance):
    mask = 2**distance
    pairs = [(source, source ^ mask) for source in range(lax.axis_size(axis))]
    return lax.ppermute(value, axis, pairs)


def slot_tables(expert_ids, route_weight, experts, capacity):
    token_count, top_count = expert_ids.shape
    pair_count = token_count * top_count
    flat_ids = expert_ids.reshape(pair_count)
    onehot = (flat_ids[:, None] == jnp.arange(experts, dtype=jnp.int32)[None, :]).astype(jnp.int32)
    before = jnp.cumsum(onehot, axis=0) - onehot
    ranks = jnp.sum(before * onehot, axis=1)
    kept = ranks < capacity
    slots = jnp.where(kept, flat_ids * capacity + ranks, 0)
    slot_ids = jnp.arange(experts * capacity, dtype=jnp.int32)
    match = (slots[None, :] == slot_ids[:, None]) & kept[None, :]
    pair_ids = jnp.arange(pair_count, dtype=jnp.int32)
    pair_of_slot = jnp.sum(jnp.where(match, pair_ids[None, :], 0), axis=1)
    filled = jnp.any(match, axis=1)
    flat_weight = route_weight.reshape(pair_count)
    weight_of_slot = jnp.sum(jnp.where(match, flat_weight[None, :], jnp.float32(0.0)), axis=1)
    return (kept, slots, pair_of_slot // top_count, filled, weight_of_slot)


def activations(gate, up, back):
    logistic = jax.nn.sigmoid(gate)
    silu = gate * logistic
    hidden = (silu * up).astype(jnp.bfloat16)
    d_gate = (back * up * logistic * (1.0 + gate * (1.0 - logistic))).astype(jnp.bfloat16)
    d_up = (back * silu).astype(jnp.bfloat16)
    return (hidden, d_gate, d_up)


def swap(value, axis, distance):
    return from_partner(value, axis, distance)


def wide(value):
    return value.astype(jnp.float32)


def dot_last(left, right):
    return lax.dot_general(left, right, CONTRACT_LAST, preferred_element_type=jnp.float32)


def dot_first(left, right):
    return lax.dot_general(left, right, CONTRACT_FIRST, preferred_element_type=jnp.float32)


def body(tokens, out_grad, route_weight, expert_ids, w_gate, w_up, w_down):
    devices_ep = lax.axis_size("ep")
    experts = devices_ep // GROUP
    token_count = tokens.shape[0]
    capacity = 6 * GROUP * token_count * TOP // (8 * devices_ep)
    quarter = D // GROUP
    short = jnp.bfloat16
    kept, slots, token_of_slot, filled, weight_of_slot = slot_tables(
        expert_ids, route_weight, experts, capacity
    )
    other_w = tuple(swap(w, "dp", 1) for w in (w_gate, w_up, w_down))
    token_ids = jnp.arange(token_count, dtype=jnp.int32)
    pick = ((token_of_slot[:, None] == token_ids[None, :]) & filled[:, None]).astype(short)
    x_slots = jnp.dot(pick, tokens, preferred_element_type=jnp.float32).astype(short)
    d_slots = (
        jnp.dot(pick, out_grad, preferred_element_type=jnp.float32) * weight_of_slot[:, None]
    ).astype(short)

    def to_owners(rows):
        shaped = rows.reshape(experts, capacity, GROUP, quarter).transpose(0, 2, 1, 3)
        return shaped.reshape(devices_ep, capacity, quarter)

    def sent(rows):
        return lax.all_to_all(to_owners(rows), "ep", split_axis=0, concat_axis=0, tiled=True)

    row_count = devices_ep * capacity
    x_own = sent(x_slots).reshape(row_count, quarter)
    d_own = sent(d_slots).reshape(row_count, quarter)
    x_other, d_other = swap(x_own, "dp", 0), swap(d_own, "dp", 0)
    core = lax.axis_index("ep") % 2
    weights = ((w_gate, w_up, w_down), other_w)
    acts = []
    for x_rows, d_rows in ((x_own, d_own), (x_other, d_other)):
        terms = [
            jnp.concatenate(
                [dot_last(x_rows, wg), dot_last(x_rows, wu), dot_last(d_rows, wd)], axis=1
            ).astype(short)
            for wg, wu, wd in weights
        ]
        give = jnp.where(core == 0, terms[1], terms[0])
        keep = jnp.where(core == 0, terms[0], terms[1])
        pair = (wide(keep) + wide(swap(give, "ep", 0))).astype(short)
        total = wide(pair) + wide(swap(pair, "ep", 1))
        width = total.shape[1] // 3
        mine = jnp.concatenate(
            activations(total[:, :width], total[:, width : 2 * width], total[:, 2 * width :]), axis=1
        )
        theirs = swap(mine, "ep", 0)
        first = jnp.where(core == 0, mine, theirs)
        second = jnp.where(core == 0, theirs, mine)
        acts.append(
            tuple(
                tuple(half[:, piece * width : (piece + 1) * width] for piece in range(3))
                for half in (first, second)
            )
        )

    def grads(half):
        (h0, g0, u0), (h1, g1, u1) = acts[0][half], acts[1][half]
        return (
            dot_first(g0, x_own) + dot_first(g1, x_other),
            dot_first(u0, x_own) + dot_first(u1, x_other),
            dot_first(h0, d_own) + dot_first(h1, d_other),
        )

    def dx(rows):
        return sum(
            jnp.dot(acts[rows][half][1], weights[half][0], preferred_element_type=jnp.float32)
            + jnp.dot(acts[rows][half][2], weights[half][1], preferred_element_type=jnp.float32)
            for half in range(2)
        )

    dx_in = swap(dx(1).astype(short), "dp", 0)
    away = tuple(swap(term.astype(short), "dp", 1) for term in grads(1))
    expert_dx = (dx(0) + wide(dx_in)).astype(short)
    grad_gate, grad_up, grad_down = (
        (own + wide(term)).astype(short) for own, term in zip(grads(0), away)
    )
    returned = lax.all_to_all(
        expert_dx.reshape(devices_ep, capacity, quarter),
        "ep",
        split_axis=0,
        concat_axis=0,
        tiled=True,
    )
    slot_rows = (
        returned.reshape(experts, GROUP, capacity, quarter)
        .transpose(0, 2, 1, 3)
        .reshape(experts * capacity, D)
    )
    in_grad = dot_first(pick, slot_rows).astype(short)
    return (in_grad, grad_gate, grad_up, grad_down)


MESH = pl.DeviceIdType.MESH
LANES = 256


def flip(index, bit):
    size = 1 << bit
    return index + size - 2 * size * lax.rem(lax.div(index, size), 2)


def expert_kernel(
    xs, ds, wg, wu, wd, slot_rows, grad_gate, grad_up, grad_down,
    x_all, d_all, w_all, give, keep, got, pair, across, act, act_t,
    term_out, term_in, term_own, dx_out, dx_in, dx_own, dx_sum,
    w_local, w_send, w_recv, self_sem, x_send, x_recv, d_send, d_recv,
    fx_send, fx_recv, fd_send, fd_recv, give_send, give_recv, pair_send, pair_recv,
    act_send, act_recv, term_send, term_recv, dx_send, dx_recv, back_send, back_recv,
):
    devices_ep, capacity, quarter = dx_sum.shape
    rows = devices_ep * capacity
    hidden = wg.shape[0]
    r, s = lax.axis_index("dp"), lax.axis_index("ep")
    core = lax.rem(s, 2)
    row_mate, weight_mate = (flip(r, 0), s), (flip(r, 1), s)
    core_mate, chip_mate = (r, flip(s, 0)), (r, flip(s, 1))
    half = devices_ep // 2
    order = sorted(range(1, devices_ep), key=lambda j: abs(j - half))

    barrier = pltpu.get_barrier_semaphore()
    peers = [row_mate, weight_mate]
    peers += [(r, lax.rem(s + j, devices_ep)) for j in range(1, devices_ep)]
    for peer in peers:
        pl.semaphore_signal(barrier, inc=1, device_id=peer, device_id_type=MESH)
    pl.semaphore_wait(barrier, len(peers))

    def remote(source, target, send, recv, peer):
        copy = pltpu.make_async_remote_copy(
            src_ref=source, dst_ref=target, send_sem=send, recv_sem=recv,
            device_id=peer, device_id_type=MESH,
        )
        copy.start()
        return copy

    def local(source, target, sem):
        copy = pltpu.make_async_copy(source, target, sem)
        copy.start()
        return copy

    def owned(ref, device):
        row = pl.multiple_of(lax.div(device, GROUP) * capacity, capacity)
        column = pl.multiple_of(lax.rem(device, GROUP) * quarter, 128)
        return ref.at[pl.ds(row, capacity), pl.ds(column, quarter)]

    sent = []
    self_copies = [
        local(owned(xs, s), x_all.at[0, s], self_sem.at[0]),
        local(owned(ds, s), d_all.at[0, s], self_sem.at[1]),
    ]
    weights = (wg, wu, wd)
    w_copies = [
        remote(w, w_all.at[1, i], w_send.at[i], w_recv.at[i], weight_mate)
        for i, w in enumerate(weights)
    ]
    own_w = [local(w, w_all.at[0, i], w_local.at[i]) for i, w in enumerate(weights)]
    x_copies, d_copies = {}, {}
    for copies, source, target, send, recv in (
        (x_copies, xs, x_all, x_send, x_recv),
        (d_copies, ds, d_all, d_send, d_recv),
    ):
        for j in order:
            peer = lax.rem(s + j, devices_ep)
            copies[j] = remote(
                owned(source, peer), target.at[0, s], send.at[j], recv.at[j], (r, peer)
            )
    passed = []
    for n, (copies, target, send, recv) in enumerate(
        ((x_copies, x_all, fx_send, fx_recv), (d_copies, d_all, fd_send, fd_recv))
    ):
        self_copies[n].wait()
        for j in [0] + order:
            if j:
                copies[j].wait_recv()
            origin = lax.rem(s + devices_ep - j, devices_ep)
            passed.append(
                remote(
                    target.at[0, origin], target.at[1, origin], send.at[j], recv.at[j], row_mate
                )
            )
    for copy in own_w:
        copy.wait()
    for copy in w_copies:
        copy.wait_recv()

    def project(k, which, out):
        for i in range(3):
            block = (x_all if i < 2 else d_all)[k].reshape(rows, quarter)
            out[k, :, i * hidden : (i + 1) * hidden] = dot_last(block, w_all[which, i]).astype(
                jnp.bfloat16
            )

    STEP = 48

    def by_rows(fn):
        def one(n, carry):
            fn(pl.ds(pl.multiple_of(n * STEP, STEP), STEP))
            return carry

        lax.fori_loop(0, rows // STEP, one, 0)

    give_copies, pair_copies, act_copies = [], [], []
    for k in range(2):
        if k == 1:
            for copy in passed:
                copy.wait_recv()
        project(k, 1 - core, give)
        give_copies.append(
            remote(give.at[k], got.at[k], give_send.at[k], give_recv.at[k], core_mate)
        )
        project(k, core, keep)
        give_copies[k].wait_recv()

        def add_pair(at, k=k):
            pair[k, at, :] = (wide(keep[k, at, :]) + wide(got[k, at, :])).astype(jnp.bfloat16)

        by_rows(add_pair)
        pair_copies.append(
            remote(pair.at[k], across.at[k], pair_send.at[k], pair_recv.at[k], chip_mate)
        )
    for k in range(2):
        pair_copies[k].wait_recv()

        def activate(at, k=k):
            total = wide(pair[k, at, :]) + wide(across[k, at, :])
            made = activations(
                total[:, :hidden], total[:, hidden : 2 * hidden], total[:, 2 * hidden :]
            )
            for i in range(3):
                act[k, core, at, i * hidden : (i + 1) * hidden] = made[i]

        by_rows(activate)
        act_copies.append(
            remote(
                act.at[k, core], act.at[k, core], act_send.at[k], act_recv.at[k], core_mate
            )
        )
    for k in range(2):
        act_copies[k].wait_recv()
        for which in (1, 0):
            act_t[which, :, k * rows : (k + 1) * rows] = act[k, which].T

    def by_columns(fn):
        def one(n, carry):
            fn(pl.ds(pl.multiple_of(n * LANES, LANES), LANES))
            return carry

        lax.fori_loop(0, quarter // LANES, one, 0)

    def term(which, i, at):
        a = (i + 1) % 3 * hidden
        block = (x_all if i < 2 else d_all)[:, :, :, at].reshape(2 * rows, LANES)
        return jnp.dot(
            act_t[which, a : a + hidden, :], block, preferred_element_type=jnp.float32
        )

    def expert_dx(k, at):
        return sum(
            jnp.dot(
                act[k, which, :, (i + 1) * hidden : (i + 2) * hidden],
                w_all[which, i, :, at],
                preferred_element_type=jnp.float32,
            )
            for which in range(2)
            for i in range(2)
        ).reshape(devices_ep, capacity, LANES)

    term_copies = []
    for i in range(3):

        def make_term(at, i=i):
            term_out[i, :, at] = term(1, i, at).astype(jnp.bfloat16)

        by_columns(make_term)
        term_copies.append(
            remote(
                term_out.at[i], term_in.at[i], term_send.at[i], term_recv.at[i], weight_mate
            )
        )
        if i == 0:

            def make_dx(at):
                dx_out[:, :, at] = expert_dx(1, at).astype(jnp.bfloat16)

            by_columns(make_dx)
            dx_copies = {}
            for j in order + [0]:
                block = lax.rem(s + j, devices_ep)
                dx_copies[j] = remote(
                    dx_out.at[block], dx_in.at[block], dx_send.at[j], dx_recv.at[j], row_mate
                )

    def own_dx(at):
        dx_own[:, :, at] = expert_dx(0, at)

    by_columns(own_dx)
    for i in range(3):

        def own_term(at, i=i):
            term_own[i, :, at] = term(0, i, at)

        by_columns(own_term)
    backs = []
    for j in order + [0]:
        block = lax.rem(s + j, devices_ep)
        dx_copies[j].wait_recv()
        dx_sum[block] = (dx_own[block] + wide(dx_in[block])).astype(jnp.bfloat16)
        if j:
            backs.append(
                remote(
                    dx_sum.at[block], owned(slot_rows, s), back_send.at[j], back_recv.at[j],
                    (r, block),
                )
            )
        else:
            last = local(dx_sum.at[block], owned(slot_rows, s), self_sem.at[2])
    for i, out in enumerate((grad_gate, grad_up, grad_down)):
        term_copies[i].wait_recv()

        def finish(at, i=i, out=out):
            out[:, at] = (term_own[i, :, at] + wide(term_in[i, :, at])).astype(jnp.bfloat16)

        by_columns(finish)
    last.wait()
    for copy in backs:
        copy.wait_recv()
    sent = w_copies + list(x_copies.values()) + list(d_copies.values()) + passed
    sent += give_copies + pair_copies + act_copies + term_copies + list(dx_copies.values())
    for copy in sent + backs:
        copy.wait_send()


def fast_body(tokens, out_grad, route_weight, expert_ids, w_gate, w_up, w_down):
    devices_ep = lax.axis_size("ep")
    experts = devices_ep // GROUP
    token_count = tokens.shape[0]
    capacity = 6 * GROUP * token_count * TOP // (8 * devices_ep)
    quarter = D // GROUP
    hidden = w_gate.shape[0]
    rows = devices_ep * capacity
    short = jnp.bfloat16
    _, _, token_of_slot, filled, weight_of_slot = slot_tables(
        expert_ids, route_weight, experts, capacity
    )
    token_ids = jnp.arange(token_count, dtype=jnp.int32)
    pick = ((token_of_slot[:, None] == token_ids[None, :]) & filled[:, None]).astype(short)
    x_slots = jnp.dot(pick, tokens, preferred_element_type=jnp.float32).astype(short)
    d_slots = (
        jnp.dot(pick, out_grad, preferred_element_type=jnp.float32) * weight_of_slot[:, None]
    ).astype(short)
    vmem = pl.BlockSpec(memory_space=pltpu.VMEM)
    hbm = pl.BlockSpec(memory_space=pl.ANY)
    grad = jax.ShapeDtypeStruct(w_gate.shape, short)
    dma = pltpu.SemaphoreType.DMA
    slot_rows, grad_gate, grad_up, grad_down = pl.pallas_call(
        expert_kernel,
        out_shape=(jax.ShapeDtypeStruct(x_slots.shape, short), grad, grad, grad),
        in_specs=[vmem, vmem, hbm, hbm, hbm],
        out_specs=(vmem, vmem, vmem, vmem),
        scratch_shapes=[
            pltpu.VMEM((2, devices_ep, capacity, quarter), short),
            pltpu.VMEM((2, devices_ep, capacity, quarter), short),
            pltpu.VMEM((2, 3, hidden, quarter), short),
            pltpu.VMEM((2, rows, 3 * hidden), short),
            pltpu.VMEM((2, rows, 3 * hidden), short),
            pltpu.VMEM((2, rows, 3 * hidden), short),
            pltpu.VMEM((2, rows, 3 * hidden), short),
            pltpu.VMEM((2, rows, 3 * hidden), short),
            pltpu.VMEM((2, 2, rows, 3 * hidden), short),
            pltpu.VMEM((2, 3 * hidden, 2 * rows), short),
            pltpu.VMEM((3, hidden, quarter), short),
            pltpu.VMEM((3, hidden, quarter), short),
            pltpu.VMEM((3, hidden, quarter), jnp.float32),
            pltpu.VMEM((devices_ep, capacity, quarter), short),
            pltpu.VMEM((devices_ep, capacity, quarter), short),
            pltpu.VMEM((devices_ep, capacity, quarter), jnp.float32),
            pltpu.VMEM((devices_ep, capacity, quarter), short),
        ]
        + [dma((3,))] * 4
        + [dma((devices_ep,))] * 8
        + [dma((2,))] * 6
        + [dma((3,))] * 2
        + [dma((devices_ep,))] * 4,
        compiler_params=pltpu.CompilerParams(
            collective_id=0, has_side_effects=True, vmem_limit_bytes=60 * 2**20
        ),
    )(x_slots, d_slots, w_gate, w_up, w_down)
    in_grad = dot_first(pick, slot_rows).astype(short)
    return (in_grad, grad_gate, grad_up, grad_down)


def solution(mesh):
    devices_ep = mesh.shape["ep"]

    def step(*arrays):
        capacity = 6 * GROUP * arrays[0].shape[0] * TOP // (8 * devices_ep)
        hidden = arrays[4].shape[0]
        fits = capacity % 48 == 0 and hidden % 128 == 0 and mesh.shape["dp"] == 4
        return (fast_body if fits else body)(*arrays)

    placed = (
        P(("dp", "ep"), None),
        P(("dp", "ep"), None),
        P(("dp", "ep"), None),
        P(("dp", "ep"), None),
        P("dp", "ep"),
        P("dp", "ep"),
        P("dp", "ep"),
    )
    return jax.shard_map(
        step,
        mesh=mesh,
        in_specs=placed,
        out_specs=(P(("dp", "ep"), None), P("dp", "ep"), P("dp", "ep"), P("dp", "ep")),
        check_vma=False,
    )
```

```python
import jax
import jax.numpy as jnp
from jax import lax
from jax.experimental import pallas as pl
from jax.experimental.pallas import tpu as pltpu
from jax.sharding import PartitionSpec as P

D = 7168
GROUP = 4
TOP = 1


CONTRACT_LAST = (((1,), (1,)), ((), ()))
CONTRACT_FIRST = (((0,), (0,)), ((), ()))


def as_sent(value):

    def short(part):
        return part.astype(jnp.bfloat16) if part.dtype == jnp.float32 else part

    return jax.tree.map(short, value)


def from_partner(value, axis, distance):
    mask = 2**distance
    pairs = [(source, source ^ mask) for source in range(lax.axis_size(axis))]
    return lax.ppermute(value, axis, pairs)


def slot_tables(expert_ids, route_weight, experts, capacity):
    token_count, top_count = expert_ids.shape
    pair_count = token_count * top_count
    flat_ids = expert_ids.reshape(pair_count)
    onehot = (flat_ids[:, None] == jnp.arange(experts, dtype=jnp.int32)[None, :]).astype(jnp.int32)
    before = jnp.cumsum(onehot, axis=0) - onehot
    ranks = jnp.sum(before * onehot, axis=1)
    kept = ranks < capacity
    slots = jnp.where(kept, flat_ids * capacity + ranks, 0)
    slot_ids = jnp.arange(experts * capacity, dtype=jnp.int32)
    match = (slots[None, :] == slot_ids[:, None]) & kept[None, :]
    pair_ids = jnp.arange(pair_count, dtype=jnp.int32)
    pair_of_slot = jnp.sum(jnp.where(match, pair_ids[None, :], 0), axis=1)
    filled = jnp.any(match, axis=1)
    flat_weight = route_weight.reshape(pair_count)
    weight_of_slot = jnp.sum(jnp.where(match, flat_weight[None, :], jnp.float32(0.0)), axis=1)
    return (kept, slots, pair_of_slot // top_count, filled, weight_of_slot)


def activations(gate, up, back):
    logistic = jax.nn.sigmoid(gate)
    silu = gate * logistic
    hidden = (silu * up).astype(jnp.bfloat16)
    d_gate = (back * up * logistic * (1.0 + gate * (1.0 - logistic))).astype(jnp.bfloat16)
    d_up = (back * silu).astype(jnp.bfloat16)
    return (hidden, d_gate, d_up)


def swap(value, axis, distance):
    return from_partner(value, axis, distance)


def wide(value):
    return value.astype(jnp.float32)


def dot_last(left, right):
    return lax.dot_general(left, right, CONTRACT_LAST, preferred_element_type=jnp.float32)


def dot_first(left, right):
    return lax.dot_general(left, right, CONTRACT_FIRST, preferred_element_type=jnp.float32)


def body(tokens, out_grad, route_weight, expert_ids, w_gate, w_up, w_down):
    devices_ep = lax.axis_size("ep")
    experts = devices_ep // GROUP
    token_count = tokens.shape[0]
    capacity = 6 * GROUP * token_count * TOP // (8 * devices_ep)
    quarter = D // GROUP
    short = jnp.bfloat16
    kept, slots, token_of_slot, filled, weight_of_slot = slot_tables(
        expert_ids, route_weight, experts, capacity
    )
    other_w = tuple(swap(w, "dp", 1) for w in (w_gate, w_up, w_down))
    token_ids = jnp.arange(token_count, dtype=jnp.int32)
    pick = ((token_of_slot[:, None] == token_ids[None, :]) & filled[:, None]).astype(short)
    x_slots = jnp.dot(pick, tokens, preferred_element_type=jnp.float32).astype(short)
    d_slots = (
        jnp.dot(pick, out_grad, preferred_element_type=jnp.float32) * weight_of_slot[:, None]
    ).astype(short)

    def to_owners(rows):
        shaped = rows.reshape(experts, capacity, GROUP, quarter).transpose(0, 2, 1, 3)
        return shaped.reshape(devices_ep, capacity, quarter)

    def sent(rows):
        return lax.all_to_all(to_owners(rows), "ep", split_axis=0, concat_axis=0, tiled=True)

    row_count = devices_ep * capacity
    x_own = sent(x_slots).reshape(row_count, quarter)
    d_own = sent(d_slots).reshape(row_count, quarter)
    x_other, d_other = swap(x_own, "dp", 0), swap(d_own, "dp", 0)
    core = lax.axis_index("ep") % 2
    weights = ((w_gate, w_up, w_down), other_w)
    acts = []
    for x_rows, d_rows in ((x_own, d_own), (x_other, d_other)):
        terms = [
            jnp.concatenate(
                [dot_last(x_rows, wg), dot_last(x_rows, wu), dot_last(d_rows, wd)], axis=1
            ).astype(short)
            for wg, wu, wd in weights
        ]
        give = jnp.where(core == 0, terms[1], terms[0])
        keep = jnp.where(core == 0, terms[0], terms[1])
        pair = (wide(keep) + wide(swap(give, "ep", 0))).astype(short)
        total = wide(pair) + wide(swap(pair, "ep", 1))
        width = total.shape[1] // 3
        mine = jnp.concatenate(
            activations(total[:, :width], total[:, width : 2 * width], total[:, 2 * width :]), axis=1
        )
        theirs = swap(mine, "ep", 0)
        first = jnp.where(core == 0, mine, theirs)
        second = jnp.where(core == 0, theirs, mine)
        acts.append(
            tuple(
                tuple(half[:, piece * width : (piece + 1) * width] for piece in range(3))
                for half in (first, second)
            )
        )

    def grads(half):
        (h0, g0, u0), (h1, g1, u1) = acts[0][half], acts[1][half]
        return (
            dot_first(g0, x_own) + dot_first(g1, x_other),
            dot_first(u0, x_own) + dot_first(u1, x_other),
            dot_first(h0, d_own) + dot_first(h1, d_other),
        )

    def dx(rows):
        return sum(
            jnp.dot(acts[rows][half][1], weights[half][0], preferred_element_type=jnp.float32)
            + jnp.dot(acts[rows][half][2], weights[half][1], preferred_element_type=jnp.float32)
            for half in range(2)
        )

    dx_in = swap(dx(1).astype(short), "dp", 0)
    away = tuple(swap(term.astype(short), "dp", 1) for term in grads(1))
    expert_dx = (dx(0) + wide(dx_in)).astype(short)
    grad_gate, grad_up, grad_down = (
        (own + wide(term)).astype(short) for own, term in zip(grads(0), away)
    )
    returned = lax.all_to_all(
        expert_dx.reshape(devices_ep, capacity, quarter),
        "ep",
        split_axis=0,
        concat_axis=0,
        tiled=True,
    )
    slot_rows = (
        returned.reshape(experts, GROUP, capacity, quarter)
        .transpose(0, 2, 1, 3)
        .reshape(experts * capacity, D)
    )
    in_grad = dot_first(pick, slot_rows).astype(short)
    return (in_grad, grad_gate, grad_up, grad_down)


MESH = pl.DeviceIdType.MESH
LANES = 256


def flip(index, bit):
    size = 1 << bit
    return index + size - 2 * size * lax.rem(lax.div(index, size), 2)


def expert_kernel(
    tokens, out_grad, pick, pick_t, scale, wg, wu, wd, in_grad, grad_gate, grad_up, grad_down,
    xs, ds, slot_rows, x_all, d_all, w_all, part, got, pair, across, act, act_t,
    term_out, term_in, term_own, dx_out, dx_in, dx_own, dx_sum,
    w_local, w_send, w_recv, self_sem, x_send, x_recv, d_send, d_recv,
    fx_send, fx_recv, fd_send, fd_recv, give_send, give_recv, pair_send, pair_recv,
    act_send, act_recv, term_send, term_recv, dx_send, dx_recv, back_send, back_recv,
):
    devices_ep, capacity, quarter = dx_sum.shape
    rows = devices_ep * capacity
    hidden = wg.shape[0]
    r, s = lax.axis_index("dp"), lax.axis_index("ep")
    core = lax.rem(s, 2)
    row_mate, weight_mate = (flip(r, 0), s), (flip(r, 1), s)
    core_mate, chip_mate = (r, flip(s, 0)), (r, flip(s, 1))
    half = devices_ep // 2
    order = sorted(range(1, devices_ep), key=lambda j: abs(j - half))

    barrier = pltpu.get_barrier_semaphore()
    peers = [row_mate, weight_mate]
    peers += [(r, lax.rem(s + j, devices_ep)) for j in range(1, devices_ep)]
    for peer in peers:
        pl.semaphore_signal(barrier, inc=1, device_id=peer, device_id_type=MESH)
    pl.semaphore_wait(barrier, len(peers))

    def remote(source, target, send, recv, peer):
        copy = pltpu.make_async_remote_copy(
            src_ref=source, dst_ref=target, send_sem=send, recv_sem=recv,
            device_id=peer, device_id_type=MESH,
        )
        copy.start()
        return copy

    def local(source, target, sem):
        copy = pltpu.make_async_copy(source, target, sem)
        copy.start()
        return copy

    def owned(ref, device):
        row = pl.multiple_of(lax.div(device, GROUP) * capacity, capacity)
        column = pl.multiple_of(lax.rem(device, GROUP) * quarter, 128)
        return ref.at[pl.ds(row, capacity), pl.ds(column, quarter)]

    WIDE = 4 * 128

    def by_slots(fn):
        def one(n, carry):
            fn(pl.ds(pl.multiple_of(n * WIDE, WIDE), WIDE))
            return carry

        lax.fori_loop(0, xs.shape[1] // WIDE, one, 0)

    def fill_x(at):
        xs[:, at] = jnp.dot(
            pick[...], tokens[:, at], preferred_element_type=jnp.float32
        ).astype(jnp.bfloat16)

    def fill_d(at):
        ds[:, at] = (
            jnp.dot(pick[...], out_grad[:, at], preferred_element_type=jnp.float32) * scale[...]
        ).astype(jnp.bfloat16)

    weights = (wg, wu, wd)
    w_copies = [
        remote(w, w_all.at[1, i], w_send.at[i], w_recv.at[i], weight_mate)
        for i, w in enumerate(weights)
    ]
    own_w = [local(w, w_all.at[0, i], w_local.at[i]) for i, w in enumerate(weights)]
    x_copies, d_copies = {}, {}
    self_copies = []
    for n, (fill, copies, source, target, send, recv) in enumerate((
        (fill_x, x_copies, xs, x_all, x_send, x_recv),
        (fill_d, d_copies, ds, d_all, d_send, d_recv),
    )):
        by_slots(fill)
        for j in order:
            peer = lax.rem(s + j, devices_ep)
            copies[j] = remote(
                owned(source, peer), target.at[0, s], send.at[j], recv.at[j], (r, peer)
            )
        self_copies.append(local(owned(source, s), target.at[0, s], self_sem.at[n]))
    passed = ([], [])

    def pass_on(n, j):
        copies, target, send, recv = (
            (x_copies, x_all, fx_send, fx_recv),
            (d_copies, d_all, fd_send, fd_recv),
        )[n]
        if j:
            copies[j].wait_recv()
        else:
            self_copies[n].wait()
        origin = lax.rem(s + devices_ep - j, devices_ep)
        passed[n].append(
            remote(target.at[0, origin], target.at[1, origin], send.at[j], recv.at[j], row_mate)
        )

    def project(k, which, pieces):
        for i in pieces:
            block = (x_all if i < 2 else d_all)[k].reshape(rows, quarter)
            part[k, which, i] = dot_last(block, w_all[which, i]).astype(jnp.bfloat16)

    STEP = 48

    def by_rows(fn):
        def one(n, carry):
            fn(pl.ds(pl.multiple_of(n * STEP, STEP), STEP))
            return carry

        lax.fori_loop(0, rows // STEP, one, 0)

    give_copies, pair_copies, act_copies = {}, {}, []
    groups = ((0, 1), (2,))

    def hand_over(k, g):
        pieces = pl.ds(groups[g][0], len(groups[g]))
        give_copies[k, g] = remote(
            part.at[k, 1 - core, pieces], got.at[k, pieces],
            give_send.at[2 * k + g], give_recv.at[2 * k + g], core_mate,
        )

    def send_pair(k, g):
        give_copies[k, g].wait_recv()

        def add_pair(at):
            for i in groups[g]:
                pair[k, i, at, :] = (wide(part[k, core, i, at, :]) + wide(got[k, i, at, :])).astype(
                    jnp.bfloat16
                )

        by_rows(add_pair)
        pieces = pl.ds(groups[g][0], len(groups[g]))
        pair_copies[k, g] = remote(
            pair.at[k, pieces], across.at[k, pieces],
            pair_send.at[2 * k + g], pair_recv.at[2 * k + g], chip_mate,
        )

    def gate_up_first():
        project(0, 0, (0, 1))

    def gate_up_second():
        for i in range(2):
            w_copies[i].wait_recv()
        project(0, 1, (0, 1))
        hand_over(0, 0)

    def gate_up_third():
        for copy in passed[0]:
            copy.wait_recv()
        project(1, 0, (0, 1))

    def gate_up_fourth():
        send_pair(0, 0)
        project(1, 1, (0, 1))
        hand_over(1, 0)

    between = {3: gate_up_first, 4: gate_up_second, 5: gate_up_third, 6: gate_up_fourth}
    for j in [0] + order:
        pass_on(0, j)
    for copy in own_w:
        copy.wait()
    for n, j in enumerate([0] + order):
        pass_on(1, j)
        if n in between:
            between[n]()
    send_pair(1, 0)
    w_copies[2].wait_recv()
    for which in range(2):
        project(0, which, (2,))
    hand_over(0, 1)
    for copy in passed[1]:
        copy.wait_recv()
    for which in range(2):
        project(1, which, (2,))
    hand_over(1, 1)
    for k in range(2):
        send_pair(k, 1)
    for k in range(2):
        for g in range(2):
            pair_copies[k, g].wait_recv()

        def activate(at, k=k):
            total = [wide(pair[k, i, at, :]) + wide(across[k, i, at, :]) for i in range(3)]
            made = activations(*total)
            for i in range(3):
                act[k, core, at, i * hidden : (i + 1) * hidden] = made[i]

        by_rows(activate)
        act_copies.append(
            remote(
                act.at[k, core], act.at[k, core], act_send.at[k], act_recv.at[k], core_mate
            )
        )

    def transpose(which):
        for k in range(2):
            act_t[which, :, k * rows : (k + 1) * rows] = act[k, which].T

    for k in range(2):
        act_copies[k].wait_recv()
    transpose(1)

    def by_columns(fn):
        def one(n, carry):
            fn(pl.ds(pl.multiple_of(n * LANES, LANES), LANES))
            return carry

        lax.fori_loop(0, quarter // LANES, one, 0)

    def term(which, i, at):
        a = (i + 1) % 3 * hidden
        block = (x_all if i < 2 else d_all)[:, :, :, at].reshape(2 * rows, LANES)
        return jnp.dot(
            act_t[which, a : a + hidden, :], block, preferred_element_type=jnp.float32
        )

    def expert_dx(k, at):
        return sum(
            jnp.dot(
                act[k, which, :, (i + 1) * hidden : (i + 2) * hidden],
                w_all[which, i, :, at],
                preferred_element_type=jnp.float32,
            )
            for which in range(2)
            for i in range(2)
        ).reshape(devices_ep, capacity, LANES)

    term_copies = []
    for i in range(3):

        def make_term(at, i=i):
            term_out[i, :, at] = term(1, i, at).astype(jnp.bfloat16)

        by_columns(make_term)
        term_copies.append(
            remote(
                term_out.at[i], term_in.at[i], term_send.at[i], term_recv.at[i], weight_mate
            )
        )
        if i == 0:

            def make_dx(at):
                dx_out[:, :, at] = expert_dx(1, at).astype(jnp.bfloat16)

            by_columns(make_dx)
            dx_copies = {}
            for j in order + [0]:
                block = lax.rem(s + j, devices_ep)
                dx_copies[j] = remote(
                    dx_out.at[block], dx_in.at[block], dx_send.at[j], dx_recv.at[j], row_mate
                )

    def own_dx(at):
        dx_own[:, :, at] = expert_dx(0, at)

    by_columns(own_dx)
    transpose(0)
    for i in range(3):

        def own_term(at, i=i):
            term_own[i, :, at] = term(0, i, at)

        by_columns(own_term)
    backs = []
    for j in order + [0]:
        block = lax.rem(s + j, devices_ep)
        dx_copies[j].wait_recv()
        dx_sum[block] = (dx_own[block] + wide(dx_in[block])).astype(jnp.bfloat16)
        if j:
            backs.append(
                remote(
                    dx_sum.at[block], owned(slot_rows, s), back_send.at[j], back_recv.at[j],
                    (r, block),
                )
            )
        else:
            last = local(dx_sum.at[block], owned(slot_rows, s), self_sem.at[2])
    last.wait()
    for copy in backs:
        copy.wait_recv()

    def fill_in(at):
        in_grad[:, at] = jnp.dot(
            pick_t[...], slot_rows[:, at], preferred_element_type=jnp.float32
        ).astype(jnp.bfloat16)

    by_slots(fill_in)
    for i, out in enumerate((grad_gate, grad_up, grad_down)):
        term_copies[i].wait_recv()

        def finish(at, i=i, out=out):
            out[:, at] = (term_own[i, :, at] + wide(term_in[i, :, at])).astype(jnp.bfloat16)

        by_columns(finish)
    sent = w_copies + list(x_copies.values()) + list(d_copies.values()) + passed[0] + passed[1]
    sent += list(give_copies.values()) + list(pair_copies.values()) + act_copies + term_copies + list(dx_copies.values())
    for copy in sent + backs:
        copy.wait_send()


def fast_body(tokens, out_grad, route_weight, expert_ids, w_gate, w_up, w_down):
    devices_ep = lax.axis_size("ep")
    experts = devices_ep // GROUP
    token_count = tokens.shape[0]
    capacity = 6 * GROUP * token_count * TOP // (8 * devices_ep)
    quarter = D // GROUP
    hidden = w_gate.shape[0]
    rows = devices_ep * capacity
    short = jnp.bfloat16
    _, _, token_of_slot, filled, weight_of_slot = slot_tables(
        expert_ids, route_weight, experts, capacity
    )
    token_ids = jnp.arange(token_count, dtype=jnp.int32)
    pick = ((token_of_slot[:, None] == token_ids[None, :]) & filled[:, None]).astype(short)
    pick_t = ((token_of_slot[None, :] == token_ids[:, None]) & filled[None, :]).astype(short)
    vmem = pl.BlockSpec(memory_space=pltpu.VMEM)
    hbm = pl.BlockSpec(memory_space=pl.ANY)
    grad = jax.ShapeDtypeStruct(w_gate.shape, short)
    dma = pltpu.SemaphoreType.DMA
    in_grad, grad_gate, grad_up, grad_down = pl.pallas_call(
        expert_kernel,
        out_shape=(jax.ShapeDtypeStruct(tokens.shape, short), grad, grad, grad),
        in_specs=[vmem, vmem, vmem, vmem, vmem, hbm, hbm, hbm],
        out_specs=(vmem, vmem, vmem, vmem),
        scratch_shapes=[
            pltpu.VMEM((experts * capacity, D), short),
            pltpu.VMEM((experts * capacity, D), short),
            pltpu.VMEM((experts * capacity, D), short),
            pltpu.VMEM((2, devices_ep, capacity, quarter), short),
            pltpu.VMEM((2, devices_ep, capacity, quarter), short),
            pltpu.VMEM((2, 3, hidden, quarter), short),
            pltpu.VMEM((2, 2, 3, rows, hidden), short),
            pltpu.VMEM((2, 3, rows, hidden), short),
            pltpu.VMEM((2, 3, rows, hidden), short),
            pltpu.VMEM((2, 3, rows, hidden), short),
            pltpu.VMEM((2, 2, rows, 3 * hidden), short),
            pltpu.VMEM((2, 3 * hidden, 2 * rows), short),
            pltpu.VMEM((3, hidden, quarter), short),
            pltpu.VMEM((3, hidden, quarter), short),
            pltpu.VMEM((3, hidden, quarter), jnp.float32),
            pltpu.VMEM((devices_ep, capacity, quarter), short),
            pltpu.VMEM((devices_ep, capacity, quarter), short),
            pltpu.VMEM((devices_ep, capacity, quarter), jnp.float32),
            pltpu.VMEM((devices_ep, capacity, quarter), short),
        ]
        + [dma((3,))] * 4
        + [dma((devices_ep,))] * 8
        + [dma((4,))] * 4
        + [dma((2,))] * 2
        + [dma((3,))] * 2
        + [dma((devices_ep,))] * 4,
        compiler_params=pltpu.CompilerParams(
            collective_id=0, has_side_effects=True, vmem_limit_bytes=60 * 2**20
        ),
    )(tokens, out_grad, pick, pick_t, weight_of_slot[:, None], w_gate, w_up, w_down)
    return (in_grad, grad_gate, grad_up, grad_down)


def solution(mesh):
    devices_ep = mesh.shape["ep"]

    def step(*arrays):
        capacity = 6 * GROUP * arrays[0].shape[0] * TOP // (8 * devices_ep)
        hidden = arrays[4].shape[0]
        fits = capacity % 48 == 0 and hidden % 128 == 0 and mesh.shape["dp"] == 4
        return (fast_body if fits else body)(*arrays)

    placed = (
        P(("dp", "ep"), None),
        P(("dp", "ep"), None),
        P(("dp", "ep"), None),
        P(("dp", "ep"), None),
        P("dp", "ep"),
        P("dp", "ep"),
        P("dp", "ep"),
    )
    return jax.shard_map(
        step,
        mesh=mesh,
        in_specs=placed,
        out_specs=(P(("dp", "ep"), None), P("dp", "ep"), P("dp", "ep"), P("dp", "ep")),
        check_vma=False,
    )
```

```python
import jax
import jax.numpy as jnp
from jax import lax
from jax.experimental import pallas as pl
from jax.experimental.pallas import tpu as pltpu
from jax.sharding import PartitionSpec as P

D = 7168
GROUP = 4
TOP = 1


CONTRACT_LAST = (((1,), (1,)), ((), ()))
CONTRACT_FIRST = (((0,), (0,)), ((), ()))


def as_sent(value):

    def short(part):
        return part.astype(jnp.bfloat16) if part.dtype == jnp.float32 else part

    return jax.tree.map(short, value)


def from_partner(value, axis, distance):
    mask = 2**distance
    pairs = [(source, source ^ mask) for source in range(lax.axis_size(axis))]
    return lax.ppermute(value, axis, pairs)


def slot_tables(expert_ids, route_weight, experts, capacity):
    token_count, top_count = expert_ids.shape
    pair_count = token_count * top_count
    flat_ids = expert_ids.reshape(pair_count)
    onehot = (flat_ids[:, None] == jnp.arange(experts, dtype=jnp.int32)[None, :]).astype(jnp.int32)
    before = jnp.cumsum(onehot, axis=0) - onehot
    ranks = jnp.sum(before * onehot, axis=1)
    kept = ranks < capacity
    slots = jnp.where(kept, flat_ids * capacity + ranks, 0)
    slot_ids = jnp.arange(experts * capacity, dtype=jnp.int32)
    match = (slots[None, :] == slot_ids[:, None]) & kept[None, :]
    pair_ids = jnp.arange(pair_count, dtype=jnp.int32)
    pair_of_slot = jnp.sum(jnp.where(match, pair_ids[None, :], 0), axis=1)
    filled = jnp.any(match, axis=1)
    flat_weight = route_weight.reshape(pair_count)
    weight_of_slot = jnp.sum(jnp.where(match, flat_weight[None, :], jnp.float32(0.0)), axis=1)
    return (kept, slots, pair_of_slot // top_count, filled, weight_of_slot)


def activations(gate, up, back):
    logistic = jax.nn.sigmoid(gate)
    silu = gate * logistic
    hidden = (silu * up).astype(jnp.bfloat16)
    d_gate = (back * up * logistic * (1.0 + gate * (1.0 - logistic))).astype(jnp.bfloat16)
    d_up = (back * silu).astype(jnp.bfloat16)
    return (hidden, d_gate, d_up)


def swap(value, axis, distance):
    return from_partner(value, axis, distance)


def wide(value):
    return value.astype(jnp.float32)


def dot_last(left, right):
    return lax.dot_general(left, right, CONTRACT_LAST, preferred_element_type=jnp.float32)


def dot_first(left, right):
    return lax.dot_general(left, right, CONTRACT_FIRST, preferred_element_type=jnp.float32)


def body(tokens, out_grad, route_weight, expert_ids, w_gate, w_up, w_down):
    devices_ep = lax.axis_size("ep")
    experts = devices_ep // GROUP
    token_count = tokens.shape[0]
    capacity = 6 * GROUP * token_count * TOP // (8 * devices_ep)
    quarter = D // GROUP
    short = jnp.bfloat16
    kept, slots, token_of_slot, filled, weight_of_slot = slot_tables(
        expert_ids, route_weight, experts, capacity
    )
    other_w = tuple(swap(w, "dp", 1) for w in (w_gate, w_up, w_down))
    token_ids = jnp.arange(token_count, dtype=jnp.int32)
    pick = ((token_of_slot[:, None] == token_ids[None, :]) & filled[:, None]).astype(short)
    x_slots = jnp.dot(pick, tokens, preferred_element_type=jnp.float32).astype(short)
    d_slots = (
        jnp.dot(pick, out_grad, preferred_element_type=jnp.float32) * weight_of_slot[:, None]
    ).astype(short)

    def to_owners(rows):
        shaped = rows.reshape(experts, capacity, GROUP, quarter).transpose(0, 2, 1, 3)
        return shaped.reshape(devices_ep, capacity, quarter)

    def sent(rows):
        return lax.all_to_all(to_owners(rows), "ep", split_axis=0, concat_axis=0, tiled=True)

    row_count = devices_ep * capacity
    x_own = sent(x_slots).reshape(row_count, quarter)
    d_own = sent(d_slots).reshape(row_count, quarter)
    x_other, d_other = swap(x_own, "dp", 0), swap(d_own, "dp", 0)
    core = lax.axis_index("ep") % 2
    weights = ((w_gate, w_up, w_down), other_w)
    acts = []
    for x_rows, d_rows in ((x_own, d_own), (x_other, d_other)):
        terms = [
            jnp.concatenate(
                [dot_last(x_rows, wg), dot_last(x_rows, wu), dot_last(d_rows, wd)], axis=1
            ).astype(short)
            for wg, wu, wd in weights
        ]
        give = jnp.where(core == 0, terms[1], terms[0])
        keep = jnp.where(core == 0, terms[0], terms[1])
        pair = (wide(keep) + wide(swap(give, "ep", 0))).astype(short)
        total = wide(pair) + wide(swap(pair, "ep", 1))
        width = total.shape[1] // 3
        mine = jnp.concatenate(
            activations(total[:, :width], total[:, width : 2 * width], total[:, 2 * width :]), axis=1
        )
        theirs = swap(mine, "ep", 0)
        first = jnp.where(core == 0, mine, theirs)
        second = jnp.where(core == 0, theirs, mine)
        acts.append(
            tuple(
                tuple(half[:, piece * width : (piece + 1) * width] for piece in range(3))
                for half in (first, second)
            )
        )

    def grads(half):
        (h0, g0, u0), (h1, g1, u1) = acts[0][half], acts[1][half]
        return (
            dot_first(g0, x_own) + dot_first(g1, x_other),
            dot_first(u0, x_own) + dot_first(u1, x_other),
            dot_first(h0, d_own) + dot_first(h1, d_other),
        )

    def dx(rows):
        return sum(
            jnp.dot(acts[rows][half][1], weights[half][0], preferred_element_type=jnp.float32)
            + jnp.dot(acts[rows][half][2], weights[half][1], preferred_element_type=jnp.float32)
            for half in range(2)
        )

    dx_in = swap(dx(1).astype(short), "dp", 0)
    away = tuple(swap(term.astype(short), "dp", 1) for term in grads(1))
    expert_dx = (dx(0) + wide(dx_in)).astype(short)
    grad_gate, grad_up, grad_down = (
        (own + wide(term)).astype(short) for own, term in zip(grads(0), away)
    )
    returned = lax.all_to_all(
        expert_dx.reshape(devices_ep, capacity, quarter),
        "ep",
        split_axis=0,
        concat_axis=0,
        tiled=True,
    )
    slot_rows = (
        returned.reshape(experts, GROUP, capacity, quarter)
        .transpose(0, 2, 1, 3)
        .reshape(experts * capacity, D)
    )
    in_grad = dot_first(pick, slot_rows).astype(short)
    return (in_grad, grad_gate, grad_up, grad_down)


MESH = pl.DeviceIdType.MESH
LANES = 256


def flip(index, bit):
    size = 1 << bit
    return index + size - 2 * size * lax.rem(lax.div(index, size), 2)


def expert_kernel(
    tokens, out_grad, pick, pick_t, scale, wg, wu, wd, in_grad, grad_gate, grad_up, grad_down,
    xs, ds, slot_rows, x_all, d_all, w_all, part, got, pair, across, act, act_t,
    term_out, term_in, term_own, dx_out, dx_in, dx_own, dx_sum,
    w_local, w_send, w_recv, self_sem, x_send, x_recv, d_send, d_recv,
    fx_send, fx_recv, fd_send, fd_recv, give_send, give_recv, pair_send, pair_recv,
    act_send, act_recv, term_send, term_recv, dx_send, dx_recv, back_send, back_recv,
):
    devices_ep, capacity, quarter = dx_sum.shape
    rows = devices_ep * capacity
    hidden = wg.shape[0]
    r, s = lax.axis_index("dp"), lax.axis_index("ep")
    core = lax.rem(s, 2)
    row_mate, weight_mate = (flip(r, 0), s), (flip(r, 1), s)
    core_mate, chip_mate = (r, flip(s, 0)), (r, flip(s, 1))
    order = list(range(devices_ep - 1, 0, -1))

    def mate(mask):
        index = s
        for bit in range(mask.bit_length()):
            if mask >> bit & 1:
                index = flip(index, bit)
        return index

    barrier = pltpu.get_barrier_semaphore()
    peers = [row_mate, weight_mate]
    peers += [(r, mate(j)) for j in range(1, devices_ep)]
    for peer in peers:
        pl.semaphore_signal(barrier, inc=1, device_id=peer, device_id_type=MESH)
    pl.semaphore_wait(barrier, len(peers))

    def remote(source, target, send, recv, peer):
        copy = pltpu.make_async_remote_copy(
            src_ref=source, dst_ref=target, send_sem=send, recv_sem=recv,
            device_id=peer, device_id_type=MESH,
        )
        copy.start()
        return copy

    def local(source, target, sem):
        copy = pltpu.make_async_copy(source, target, sem)
        copy.start()
        return copy

    def owned(ref, device):
        row = pl.multiple_of(lax.div(device, GROUP) * capacity, capacity)
        column = pl.multiple_of(lax.rem(device, GROUP) * quarter, 128)
        return ref.at[pl.ds(row, capacity), pl.ds(column, quarter)]

    WIDE = 4 * 128

    def by_slots(fn):
        def one(n, carry):
            fn(pl.ds(pl.multiple_of(n * WIDE, WIDE), WIDE))
            return carry

        lax.fori_loop(0, xs.shape[1] // WIDE, one, 0)

    def fill_x(at):
        xs[:, at] = jnp.dot(
            pick[...], tokens[:, at], preferred_element_type=jnp.float32
        ).astype(jnp.bfloat16)

    def fill_d(at):
        ds[:, at] = (
            jnp.dot(pick[...], out_grad[:, at], preferred_element_type=jnp.float32) * scale[...]
        ).astype(jnp.bfloat16)

    weights = (wg, wu, wd)
    w_copies = [
        remote(w, w_all.at[1, i], w_send.at[i], w_recv.at[i], weight_mate)
        for i, w in enumerate(weights)
    ]
    own_w = [local(w, w_all.at[0, i], w_local.at[i]) for i, w in enumerate(weights)]
    x_copies, d_copies = {}, {}
    self_copies = []
    for n, (fill, copies, source, target, send, recv) in enumerate((
        (fill_x, x_copies, xs, x_all, x_send, x_recv),
        (fill_d, d_copies, ds, d_all, d_send, d_recv),
    )):
        by_slots(fill)
        for j in order:
            peer = mate(j)
            copies[j] = remote(
                owned(source, peer), target.at[0, s], send.at[j], recv.at[j], (r, peer)
            )
        self_copies.append(local(owned(source, s), target.at[0, s], self_sem.at[n]))
    passed = ([], [])

    def pass_on(n, j):
        copies, target, send, recv = (
            (x_copies, x_all, fx_send, fx_recv),
            (d_copies, d_all, fd_send, fd_recv),
        )[n]
        if j:
            copies[j].wait_recv()
        else:
            self_copies[n].wait()
        origin = mate(j)
        passed[n].append(
            remote(target.at[0, origin], target.at[1, origin], send.at[j], recv.at[j], row_mate)
        )

    def project(k, which, pieces):
        for i in pieces:
            block = (x_all if i < 2 else d_all)[k].reshape(rows, quarter)
            part[k, which, i] = dot_last(block, w_all[which, i]).astype(jnp.bfloat16)

    STEP = 48

    def by_rows(fn):
        def one(n, carry):
            fn(pl.ds(pl.multiple_of(n * STEP, STEP), STEP))
            return carry

        lax.fori_loop(0, rows // STEP, one, 0)

    give_copies, pair_copies, act_copies = {}, {}, []
    groups = ((0, 1), (2,))

    def hand_over(k, g):
        pieces = pl.ds(groups[g][0], len(groups[g]))
        give_copies[k, g] = remote(
            part.at[k, 1 - core, pieces], got.at[k, pieces],
            give_send.at[2 * k + g], give_recv.at[2 * k + g], core_mate,
        )

    def send_pair(k, g):
        give_copies[k, g].wait_recv()

        def add_pair(at):
            for i in groups[g]:
                pair[k, i, at, :] = (wide(part[k, core, i, at, :]) + wide(got[k, i, at, :])).astype(
                    jnp.bfloat16
                )

        by_rows(add_pair)
        pieces = pl.ds(groups[g][0], len(groups[g]))
        pair_copies[k, g] = remote(
            pair.at[k, pieces], across.at[k, pieces],
            pair_send.at[2 * k + g], pair_recv.at[2 * k + g], chip_mate,
        )

    def gate_up_first():
        project(0, 0, (0, 1))

    def gate_up_second():
        for i in range(2):
            w_copies[i].wait_recv()
        project(0, 1, (0, 1))
        hand_over(0, 0)

    def gate_up_third():
        for copy in passed[0]:
            copy.wait_recv()
        project(1, 0, (0, 1))

    def gate_up_fourth():
        send_pair(0, 0)
        project(1, 1, (0, 1))
        hand_over(1, 0)

    near, far = list(range(GROUP)), list(range(GROUP, devices_ep))[::-1]
    arrivals = [(0, j) for j in near]
    for n, j in enumerate(far):
        arrivals.append((0, j))
        if 0 < n <= GROUP:
            arrivals.append((1, near[n - 1]))
    arrivals += [(1, j) for j in near if (1, j) not in arrivals]
    for n, j in arrivals:
        pass_on(n, j)
    for copy in own_w:
        copy.wait()
    gate_up_first()
    steps = [gate_up_second, gate_up_third, gate_up_fourth]
    for n, j in enumerate(far):
        pass_on(1, j)
        if n < len(steps):
            steps[n]()
    send_pair(1, 0)
    w_copies[2].wait_recv()
    for which in range(2):
        project(0, which, (2,))
    hand_over(0, 1)
    for copy in passed[1]:
        copy.wait_recv()
    for which in range(2):
        project(1, which, (2,))
    hand_over(1, 1)
    for k in range(2):
        send_pair(k, 1)
    for k in range(2):
        for g in range(2):
            pair_copies[k, g].wait_recv()

        def activate(at, k=k):
            total = [wide(pair[k, i, at, :]) + wide(across[k, i, at, :]) for i in range(3)]
            made = activations(*total)
            for i in range(3):
                act[k, core, at, i * hidden : (i + 1) * hidden] = made[i]

        by_rows(activate)
        act_copies.append(
            remote(
                act.at[k, core], act.at[k, core], act_send.at[k], act_recv.at[k], core_mate
            )
        )

    def transpose(which):
        for k in range(2):
            act_t[which, :, k * rows : (k + 1) * rows] = act[k, which].T

    for k in range(2):
        act_copies[k].wait_recv()
    transpose(1)

    def by_columns(fn):
        def one(n, carry):
            fn(pl.ds(pl.multiple_of(n * LANES, LANES), LANES))
            return carry

        lax.fori_loop(0, quarter // LANES, one, 0)

    def term(which, i, at):
        a = (i + 1) % 3 * hidden
        block = (x_all if i < 2 else d_all)[:, :, :, at].reshape(2 * rows, LANES)
        return jnp.dot(
            act_t[which, a : a + hidden, :], block, preferred_element_type=jnp.float32
        )

    def expert_dx(k, at):
        return sum(
            jnp.dot(
                act[k, which, :, (i + 1) * hidden : (i + 2) * hidden],
                w_all[which, i, :, at],
                preferred_element_type=jnp.float32,
            )
            for which in range(2)
            for i in range(2)
        ).reshape(devices_ep, capacity, LANES)

    term_copies = []
    for i in range(3):

        def make_term(at, i=i):
            term_out[i, :, at] = term(1, i, at).astype(jnp.bfloat16)

        by_columns(make_term)
        term_copies.append(
            remote(
                term_out.at[i], term_in.at[i], term_send.at[i], term_recv.at[i], weight_mate
            )
        )
        if i == 0:

            def make_dx(at):
                dx_out[:, :, at] = expert_dx(1, at).astype(jnp.bfloat16)

            by_columns(make_dx)
            dx_copies = {}
            for j in order + [0]:
                block = mate(j)
                dx_copies[j] = remote(
                    dx_out.at[block], dx_in.at[block], dx_send.at[j], dx_recv.at[j], row_mate
                )

    def own_dx(at):
        dx_own[:, :, at] = expert_dx(0, at)

    by_columns(own_dx)
    transpose(0)
    for i in range(3):

        def own_term(at, i=i):
            term_own[i, :, at] = term(0, i, at)

        by_columns(own_term)
    backs = []
    for j in order + [0]:
        block = mate(j)
        dx_copies[j].wait_recv()
        dx_sum[block] = (dx_own[block] + wide(dx_in[block])).astype(jnp.bfloat16)
        if j:
            backs.append(
                remote(
                    dx_sum.at[block], owned(slot_rows, s), back_send.at[j], back_recv.at[j],
                    (r, block),
                )
            )
        else:
            last = local(dx_sum.at[block], owned(slot_rows, s), self_sem.at[2])
    def take_back():
        last.wait()
        for copy in backs:
            copy.wait_recv()

        def fill_in(at):
            in_grad[:, at] = jnp.dot(
                pick_t[...], slot_rows[:, at], preferred_element_type=jnp.float32
            ).astype(jnp.bfloat16)

        by_slots(fill_in)

    for i, out in enumerate((grad_gate, grad_up, grad_down)):
        if i == 2:
            take_back()
        term_copies[i].wait_recv()

        def finish(at, i=i, out=out):
            out[:, at] = (term_own[i, :, at] + wide(term_in[i, :, at])).astype(jnp.bfloat16)

        by_columns(finish)
    sent = w_copies + list(x_copies.values()) + list(d_copies.values()) + passed[0] + passed[1]
    sent += list(give_copies.values()) + list(pair_copies.values()) + act_copies + term_copies + list(dx_copies.values())
    for copy in sent + backs:
        copy.wait_send()


def fast_body(tokens, out_grad, route_weight, expert_ids, w_gate, w_up, w_down):
    devices_ep = lax.axis_size("ep")
    experts = devices_ep // GROUP
    token_count = tokens.shape[0]
    capacity = 6 * GROUP * token_count * TOP // (8 * devices_ep)
    quarter = D // GROUP
    hidden = w_gate.shape[0]
    rows = devices_ep * capacity
    short = jnp.bfloat16
    _, _, token_of_slot, filled, weight_of_slot = slot_tables(
        expert_ids, route_weight, experts, capacity
    )
    token_ids = jnp.arange(token_count, dtype=jnp.int32)
    pick = ((token_of_slot[:, None] == token_ids[None, :]) & filled[:, None]).astype(short)
    pick_t = ((token_of_slot[None, :] == token_ids[:, None]) & filled[None, :]).astype(short)
    vmem = pl.BlockSpec(memory_space=pltpu.VMEM)
    hbm = pl.BlockSpec(memory_space=pl.ANY)
    grad = jax.ShapeDtypeStruct(w_gate.shape, short)
    dma = pltpu.SemaphoreType.DMA
    in_grad, grad_gate, grad_up, grad_down = pl.pallas_call(
        expert_kernel,
        out_shape=(jax.ShapeDtypeStruct(tokens.shape, short), grad, grad, grad),
        in_specs=[vmem, vmem, vmem, vmem, vmem, hbm, hbm, hbm],
        out_specs=(vmem, vmem, vmem, vmem),
        scratch_shapes=[
            pltpu.VMEM((experts * capacity, D), short),
            pltpu.VMEM((experts * capacity, D), short),
            pltpu.VMEM((experts * capacity, D), short),
            pltpu.VMEM((2, devices_ep, capacity, quarter), short),
            pltpu.VMEM((2, devices_ep, capacity, quarter), short),
            pltpu.VMEM((2, 3, hidden, quarter), short),
            pltpu.VMEM((2, 2, 3, rows, hidden), short),
            pltpu.VMEM((2, 3, rows, hidden), short),
            pltpu.VMEM((2, 3, rows, hidden), short),
            pltpu.VMEM((2, 3, rows, hidden), short),
            pltpu.VMEM((2, 2, rows, 3 * hidden), short),
            pltpu.VMEM((2, 3 * hidden, 2 * rows), short),
            pltpu.VMEM((3, hidden, quarter), short),
            pltpu.VMEM((3, hidden, quarter), short),
            pltpu.VMEM((3, hidden, quarter), jnp.float32),
            pltpu.VMEM((devices_ep, capacity, quarter), short),
            pltpu.VMEM((devices_ep, capacity, quarter), short),
            pltpu.VMEM((devices_ep, capacity, quarter), jnp.float32),
            pltpu.VMEM((devices_ep, capacity, quarter), short),
        ]
        + [dma((3,))] * 4
        + [dma((devices_ep,))] * 8
        + [dma((4,))] * 4
        + [dma((2,))] * 2
        + [dma((3,))] * 2
        + [dma((devices_ep,))] * 4,
        compiler_params=pltpu.CompilerParams(
            collective_id=0, has_side_effects=True, vmem_limit_bytes=60 * 2**20
        ),
    )(tokens, out_grad, pick, pick_t, weight_of_slot[:, None], w_gate, w_up, w_down)
    return (in_grad, grad_gate, grad_up, grad_down)


def solution(mesh):
    devices_ep = mesh.shape["ep"]

    def step(*arrays):
        capacity = 6 * GROUP * arrays[0].shape[0] * TOP // (8 * devices_ep)
        hidden = arrays[4].shape[0]
        fits = capacity % 48 == 0 and hidden % 128 == 0 and mesh.shape["dp"] == 4
        return (fast_body if fits else body)(*arrays)

    placed = (
        P(("dp", "ep"), None),
        P(("dp", "ep"), None),
        P(("dp", "ep"), None),
        P(("dp", "ep"), None),
        P("dp", "ep"),
        P("dp", "ep"),
        P("dp", "ep"),
    )
    return jax.shard_map(
        step,
        mesh=mesh,
        in_specs=placed,
        out_specs=(P(("dp", "ep"), None), P("dp", "ep"), P("dp", "ep"), P("dp", "ep")),
        check_vma=False,
    )
```
